32 devices in a mesh: groups: 2 (over x), samp: 16 (over z, y, core).
Axes of the slice: x: 2, y: 2, z: 4, core: 2. Of those that a mesh axis runs over, the one named last changes fastest.
Arguments:
- dosage: bfloat16 [8192, 8192], P(('groups', 'samp')), parts along dimension 0, may hold values from 0 to 2
- covariates: bfloat16 [8192, 96], P(('groups', 'samp')), parts along dimension 0, may hold values from -8 to 8
- expression: bfloat16 [8192, 8192], P('groups', 'samp'), parts along dimension 0, may hold values from -10 to 10
- block_index: int32 [4, 1024], P('groups'), parts along dimension 0, may hold values from 0 to 8191
- expr_row: int32 [8192], P('groups'), parts along dimension 0, may hold values from 0 to 4095, each once
Outputs:
- zscore: float32 [4096, 8192], P('groups', 'samp'), parts along dimension 0
The draws below stay inside these ranges and needn't reach their ends.
There are 2 independent parts, one for each index of `groups`. The reference program is written for one: setup_inputs(seed, part) draws one part's arguments, and reference() takes and returns one part's arrays. A program takes and returns all parts, laid end to end along the dimension named above; each array names one. Nothing has to cross between parts.
Inputs may be any that keep to these rules, and one draw needn't show every extreme that they name: `expr_row`: every expression row appears once.
All inputs are finite; a program needn't handle non-finite values.
Results may differ from the reference program's by a relative error of at most 0.0029.
Values may be sent and summed in bfloat16 or wider, within the bound.
A program may use at most 192 MiB of HBM per device.

```python
import math
import jax
import jax.numpy as jnp
from jax import lax

K = 96
V = 1024
BLOCKS = 2
VPANEL = 8192
NSAMP = 4096
GENES = 8192


def covariate_base(key):
    first = jax.random.fold_in(key, 11)
    normal_part = jax.random.normal(first, (NSAMP, K), jnp.float32)
    rising = 1.0 + 2.0 * jnp.arange(NSAMP, dtype=jnp.float32) / NSAMP
    return jnp.clip(normal_part * rising[:, None], -8.0, 8.0)


def draw_covariates(key, part):
    return covariate_base(key).astype(jnp.bfloat16)


def draw_dosage(key, part):
    base = covariate_base(key)
    loading = jax.random.normal(jax.random.fold_in(key, 21), (K, VPANEL), jnp.float32)
    noise_key = jax.random.fold_in(key, 22)
    noise = jax.random.uniform(noise_key, (NSAMP, VPANEL), jnp.float32, -0.6, 0.6)
    shared = jnp.dot(base, loading) * (0.3 / K ** 0.5)
    return jnp.clip(1.0 + shared + noise, 0.0, 2.0).astype(jnp.bfloat16)


def draw_expression(key, part):
    base = covariate_base(key)
    loading = jax.random.normal(jax.random.fold_in(key, 31), (K, GENES), jnp.float32)
    noise_key = jax.random.fold_in(key, 32)
    noise = jax.random.normal(noise_key, (NSAMP, GENES), jnp.float32)
    shared = jnp.dot(base, loading) * (0.5 / K ** 0.5)
    return jnp.clip(shared + noise, -10.0, 10.0).astype(jnp.bfloat16)


def plant(entries, own_key, least, high):
    place = [jax.random.randint(jax.random.fold_in(own_key, axis), (), 0, length) for axis, length in enumerate(entries.shape)]
    widest = entries.shape.index(max(entries.shape))
    beside = place[:widest] + [(place[widest] + 1) % entries.shape[widest]] + place[widest + 1:]
    return entries.at[tuple(place)].set(least).at[tuple(beside)].set(high)


def setup_inputs(seed: int = 0, part: int = 0) -> dict:
    key_list = jax.random.split(jax.random.key(seed), 6)
    part_keys = jax.random.split(jax.random.fold_in(key_list[5], part), 6)
    dosage = draw_dosage(jax.random.fold_in(jax.random.fold_in(key_list[5], part), 71), part)
    covariates = draw_covariates(jax.random.fold_in(jax.random.fold_in(key_list[5], part), 71), part)
    expression = draw_expression(jax.random.fold_in(jax.random.fold_in(key_list[5], part), 71), part)
    block_index = plant(jax.random.randint(part_keys[3], (BLOCKS, V), 0, VPANEL), jax.random.fold_in(part_keys[3], 1), 0, VPANEL - 1).astype(jnp.int32)
    expr_row = jax.random.permutation(part_keys[4], NSAMP).astype(jnp.int32)
    return dict(dosage=dosage, covariates=covariates, expression=expression, block_index=block_index, expr_row=expr_row)


epsilon = 1e-06

def reference(dosage, covariates, expression, block_index, expr_row):
    gram = jnp.dot(covariates.T.astype(jnp.float32), covariates.astype(jnp.float32), preferred_element_type=jnp.float32)
    factor = jnp.linalg.cholesky(gram)
    matched = jnp.take(expression, expr_row, axis=0)
    panel_norm = lax.optimization_barrier(jnp.sum(jnp.square(expression.astype(jnp.float32)), axis=0))
    cov_float = covariates.astype(jnp.float32)
    scale = math.sqrt(NSAMP - K - 1)
    results = []
    for block in range(BLOCKS):
        picked = jnp.take(dosage, block_index[block], axis=1)
        loads = jnp.dot(covariates.T.astype(jnp.float32), picked.astype(jnp.float32), preferred_element_type=jnp.float32)
        coeffs = jax.scipy.linalg.cho_solve((factor, True), loads)
        fitted = jnp.dot(cov_float, coeffs, precision=lax.Precision.HIGHEST)
        resid = (picked.astype(jnp.float32) - fitted).astype(jnp.bfloat16)
        resid_norm = lax.optimization_barrier(jnp.sum(jnp.square(resid.astype(jnp.float32)), axis=0))
        products = jnp.dot(resid.T.astype(jnp.float32), matched.astype(jnp.float32), preferred_element_type=jnp.float32)
        results.append(scale * products * lax.rsqrt(resid_norm + epsilon)[:, None] * lax.rsqrt(panel_norm + epsilon)[None, :])
    return jnp.concatenate(results, axis=0)
```

```python
import functools
import math

import jax
import jax.numpy as jnp
from jax import lax
from jax.experimental import pallas as pl
from jax.experimental.pallas import tpu as pltpu
from jax.sharding import PartitionSpec as P

epsilon = 1e-06
MESH = pl.DeviceIdType.MESH
CHUNKS = 4


def exchange(n, p_ref, c_ref, expr_ref, row_ref, outp, outc, outm, norm_ref, ef, mf,
             send_sem, recv_sem, local_sem):
    depth = n // 4
    me = lax.axis_index("samp")
    z, y, core = me // 4, (me // 2) % 2, me % 2
    group = lax.axis_index("groups")
    width = p_ref.shape[0] // CHUNKS
    here = p_ref.shape[1]

    def index(zz, yy, cc):
        return (zz * 2 + yy) * 2 + cc

    def target(s):
        return (group, s)

    y_peer = index(z, 1 - y, core)
    core_peer = index(z, y, 1 - core)
    z_peers = [index(lax.rem(z + j, depth), y, core) for j in range(1, depth)]
    z_from = [index(lax.rem(z + depth - j, depth), y, core) for j in range(1, depth)]

    barrier = pltpu.get_barrier_semaphore()
    for peer in [y_peer, core_peer] + z_peers:
        pl.semaphore_signal(barrier, inc=1, device_id=target(peer), device_id_type=MESH)
    pl.semaphore_wait(barrier, depth + 1)

    pieces = CHUNKS + 1

    def stripe(owner):
        return pl.ds(pl.multiple_of(owner * here, here), here)

    def dst(piece, owner):
        if piece == 0:
            return outc.at[:, stripe(owner)]
        return outp.at[pl.ds((piece - 1) * width, width), stripe(owner)]

    def own(piece):
        if piece == 0:
            return c_ref
        return p_ref.at[pl.ds((piece - 1) * width, width), :]

    started = []

    def send(piece, owner, peer, src):
        k = len(started)
        copy = pltpu.make_async_remote_copy(
            src_ref=src, dst_ref=dst(piece, owner), send_sem=send_sem.at[k],
            recv_sem=recv_sem.at[piece, owner], device_id=target(peer), device_id_type=MESH)
        copy.start()
        started.append(copy)

    def arrive(piece, owner):
        pltpu.make_async_remote_copy(
            src_ref=own(piece), dst_ref=dst(piece, owner), send_sem=send_sem.at[0],
            recv_sem=recv_sem.at[piece, owner], device_id=target(y_peer),
            device_id_type=MESH).wait_recv()

    locals_ = []
    for piece in range(pieces):
        for peer in z_peers:
            send(piece, me, peer, own(piece))
        send(piece, me, y_peer, own(piece))
        send(piece, me, core_peer, own(piece))
        keep = pltpu.make_async_copy(own(piece), dst(piece, me), local_sem.at[piece])
        keep.start()
        locals_.append(keep)

    samples = expr_ref.shape[0]
    step = samples // 16
    norm_ref[...] = jnp.zeros_like(norm_ref)

    def widen(i, _):
        rows = pl.ds(pl.multiple_of(i * step, step), step)
        x = expr_ref[rows, :].astype(jnp.float32)
        ef[rows, :] = x
        norm_ref[...] += jnp.sum(x * x, axis=0, keepdims=True)
        return 0

    lax.fori_loop(0, 16, widen, 0)

    def match(low, high):
        def body(i, _):
            for u in range(16):
                j = i * 16 + u
                mf[pl.ds(u, 1), :] = ef[pl.ds(row_ref[j], 1), :]
            outm[pl.ds(pl.multiple_of(i * 16, 16), 16), :] = mf[...].astype(jnp.bfloat16)
            return 0
        lax.fori_loop(low, high, body, 0)

    spans = samples // 16
    cuts = [spans * p // pieces for p in range(pieces + 1)]
    for piece in range(pieces):
        arrive(piece, y_peer)
        send(piece, y_peer, core_peer, dst(piece, y_peer))
        for src in z_from:
            arrive(piece, src)
            send(piece, src, y_peer, dst(piece, src))
            send(piece, src, core_peer, dst(piece, src))
        if piece:
            late_y(piece - 1, z_from, arrive, send, core_peer, y, dst)
        match(cuts[piece], cuts[piece + 1])
    late_y(pieces - 1, z_from, arrive, send, core_peer, y, dst)
    for piece in range(pieces):
        for owner_z in range(depth):
            for owner_y in range(2):
                arrive(piece, index(owner_z, owner_y, 1 - core))
    for copy in started:
        copy.wait_send()
    for keep in locals_:
        keep.wait()


def late_y(piece, z_from, arrive, send, core_peer, y, dst):
    for src in z_from:
        other = src + 2 - 4 * y
        arrive(piece, other)
        send(piece, other, core_peer, dst(piece, other))


def finish(scale, p_ref, c_ref, k_ref, m_ref, norm_ref, out_ref, sums, sq):
    step, steps = pl.program_id(1), pl.num_programs(1)
    span = p_ref.shape[1]
    fitted = jnp.dot(k_ref[...], c_ref[...], preferred_element_type=jnp.float32)
    resid = (p_ref[...].astype(jnp.float32) - fitted).astype(jnp.bfloat16)
    wide = resid.astype(jnp.float32)
    rows = pl.ds(pl.multiple_of(step * span, span), span)
    part = jnp.dot(resid, m_ref[rows, :], preferred_element_type=jnp.float32)
    norm = jnp.sum(wide * wide, axis=1, keepdims=True)

    @pl.when(step == 0)
    def _():
        sums[...] = part
        sq[...] = norm

    @pl.when(step > 0)
    def _():
        sums[...] += part
        sq[...] += norm

    @pl.when(step == steps - 1)
    def _():
        out_ref[...] = (scale * sums[...] * lax.rsqrt(sq[...] + epsilon)
                        * lax.rsqrt(norm_ref[...] + epsilon))


def terms(x):
    first = lax.reduce_precision(x, 8, 7)
    rest = x - first
    second = lax.reduce_precision(rest, 8, 7)
    return [t.astype(jnp.bfloat16) for t in (first, second, rest - second)]


def local(n, dosage, covariates, expression, block_index, expr_row):
    blocks, block_width = block_index.shape
    covars = covariates.shape[1]
    here = covariates.shape[0]
    samples, genes = expression.shape
    variants = blocks * block_width
    scale = math.sqrt(samples - covars - 1)

    picked = jnp.take(dosage, block_index.reshape(-1), axis=1).T
    vmem = pl.BlockSpec(memory_space=pltpu.VMEM)
    anywhere = pl.BlockSpec(memory_space=pl.ANY)
    depth = n // 4
    pieces = CHUNKS + 1
    sends = pieces * (depth - 1 + 2 + 1 + 2 * (depth - 1) + depth - 1)
    everyone, covs, matched, panel_norm = pl.pallas_call(
        functools.partial(exchange, n),
        out_shape=(
            jax.ShapeDtypeStruct((variants, samples), jnp.bfloat16),
            jax.ShapeDtypeStruct((covars, samples), jnp.bfloat16),
            jax.ShapeDtypeStruct((samples, genes), jnp.bfloat16),
            jax.ShapeDtypeStruct((1, genes), jnp.float32),
        ),
        in_specs=[vmem, vmem, vmem, pl.BlockSpec(memory_space=pltpu.SMEM)],
        out_specs=(anywhere, anywhere, vmem, vmem),
        scratch_shapes=[
            pltpu.VMEM((samples, genes), jnp.float32),
            pltpu.VMEM((16, genes), jnp.float32),
            pltpu.SemaphoreType.DMA((sends,)),
            pltpu.SemaphoreType.DMA((pieces, n)),
            pltpu.SemaphoreType.DMA((pieces,)),
        ],
        compiler_params=pltpu.CompilerParams(
            collective_id=0, has_side_effects=True, vmem_limit_bytes=40 * 2**20),
    )(picked, covariates.T, expression, expr_row)

    gram = jnp.einsum("is,js->ij", covs, covs, preferred_element_type=jnp.float32)
    loads = jnp.einsum("is,vs->iv", covs, everyone, preferred_element_type=jnp.float32)
    factor = jnp.linalg.cholesky(gram)
    coeffs = jax.scipy.linalg.cho_solve((factor, True), loads)
    parts = jnp.concatenate(terms(coeffs.T), axis=1)
    covs3 = jnp.concatenate([covs] * 3, axis=0)
    tile, span = 512, min(1024, samples)
    return pl.pallas_call(
        functools.partial(finish, scale),
        out_shape=jax.ShapeDtypeStruct((variants, genes), jnp.float32),
        grid=(variants // tile, samples // span),
        in_specs=[
            pl.BlockSpec((tile, span), lambda i, j: (i, j)),
            pl.BlockSpec((3 * covars, span), lambda i, j: (0, j)),
            pl.BlockSpec((tile, 3 * covars), lambda i, j: (i, 0)),
            pl.BlockSpec((samples, genes), lambda i, j: (0, 0)),
            pl.BlockSpec((1, genes), lambda i, j: (0, 0)),
        ],
        out_specs=pl.BlockSpec((tile, genes), lambda i, j: (i, 0)),
        scratch_shapes=[
            pltpu.VMEM((tile, genes), jnp.float32),
            pltpu.VMEM((tile, 1), jnp.float32),
        ],
        compiler_params=pltpu.CompilerParams(vmem_limit_bytes=40 * 2**20),
    )(everyone, covs3, parts, matched, panel_norm)


def solution(mesh):
    placed = (
        P(("groups", "samp"), None),
        P(("groups", "samp"), None),
        P("groups", "samp"),
        P("groups", None),
        P("groups"),
    )
    return jax.shard_map(
        functools.partial(local, mesh.shape["samp"]),
        mesh=mesh, in_specs=placed, out_specs=P("groups", "samp"), check_vma=False
    )
```

```python
import functools
import math

import jax
import jax.numpy as jnp
from jax import lax
from jax.experimental import pallas as pl
from jax.experimental.pallas import tpu as pltpu
from jax.sharding import PartitionSpec as P

epsilon = 1e-06
MESH = pl.DeviceIdType.MESH
CHUNKS = 4
SPAN = 1024


def exchange(n, scale, p_ref, c_ref, expr_ref, row_ref, out_ref, panel, covs, matched,
             ef, mf, norm_ref, gram, right, lower, lower_scaled, sq, send_sem, recv_sem):
    depth = n // 4
    me = lax.axis_index("samp")
    z, y, core = me // 4, (me // 2) % 2, me % 2
    group = lax.axis_index("groups")
    width = p_ref.shape[0] // CHUNKS
    here = p_ref.shape[1]
    samples = expr_ref.shape[0]
    covars = c_ref.shape[0]

    def index(zz, yy, cc):
        return (zz * 2 + yy) * 2 + cc

    def target(s):
        return (group, s)

    y_peer = index(z, 1 - y, core)
    core_peer = index(z, y, 1 - core)
    z_peers = [index(lax.rem(z + j, depth), y, core) for j in range(1, depth)]
    z_from = [index(lax.rem(z + depth - j, depth), y, core) for j in range(1, depth)]

    barrier = pltpu.get_barrier_semaphore()
    for peer in [y_peer, core_peer] + z_peers:
        pl.semaphore_signal(barrier, inc=1, device_id=target(peer), device_id_type=MESH)
    pl.semaphore_wait(barrier, depth + 1)

    pieces = CHUNKS + 1

    def stripe(owner):
        return pl.ds(pl.multiple_of(owner * here, here), here)

    def dst(piece, owner):
        if piece == 0:
            return covs.at[:, stripe(owner)]
        return panel.at[pl.ds((piece - 1) * width, width), stripe(owner)]

    def own(piece):
        if piece == 0:
            return c_ref
        return p_ref.at[pl.ds((piece - 1) * width, width), :]

    started = []

    def send(piece, owner, peer, src):
        k = len(started)
        copy = pltpu.make_async_remote_copy(
            src_ref=src, dst_ref=dst(piece, owner), send_sem=send_sem.at[k],
            recv_sem=recv_sem.at[piece, owner], device_id=target(peer), device_id_type=MESH)
        copy.start()
        started.append(copy)

    def arrive(piece, owner):
        pltpu.make_async_remote_copy(
            src_ref=own(piece), dst_ref=dst(piece, owner), send_sem=send_sem.at[0],
            recv_sem=recv_sem.at[piece, owner], device_id=target(y_peer),
            device_id_type=MESH).wait_recv()

    for piece in range(pieces):
        for peer in z_peers:
            send(piece, me, peer, own(piece))
        send(piece, me, y_peer, own(piece))
        send(piece, me, core_peer, own(piece))
    covs[:, stripe(me)] = c_ref[...]
    panel[:, stripe(me)] = p_ref[...]

    step = samples // 16
    lanes = ef.shape[1]
    norm_ref[...] = jnp.zeros_like(norm_ref)

    def widen(part):
        genes = slice(part * lanes, (part + 1) * lanes)

        def body(i, _):
            rows = pl.ds(pl.multiple_of(i * step, step), step)
            x = expr_ref[rows, genes].astype(jnp.float32)
            ef[rows, :] = x
            norm_ref[:, genes] += jnp.sum(x * x, axis=0, keepdims=True)
            return 0

        lax.fori_loop(0, 16, body, 0)

    def match(part, low, high):
        genes = slice(part * lanes, (part + 1) * lanes)

        def body(i, _):
            for u in range(16):
                j = i * 16 + u
                mf[pl.ds(u, 1), :] = ef[pl.ds(row_ref[j], 1), :]
            rows = pl.ds(pl.multiple_of(i * 16, 16), 16)
            matched[rows, genes] = mf[...].astype(jnp.bfloat16)
            return 0

        lax.fori_loop(low, high, body, 0)

    def late(piece):
        for src in z_from:
            other = src + 2 - 4 * y
            arrive(piece, other)
            send(piece, other, core_peer, dst(piece, other))

    span = min(SPAN, samples)
    spans = samples // span
    columns = (((1,), (1,)), ((), ()))

    def cut(j):
        return pl.ds(pl.multiple_of(j * span, span), span)

    def eliminate():
        gram[...] = jnp.zeros_like(gram)

        def add(j, _):
            c = covs[:, cut(j)]
            gram[...] += lax.dot_general(c, c, columns, preferred_element_type=jnp.float32)
            return 0

        lax.fori_loop(0, spans, add, 0)
        row = lax.broadcasted_iota(jnp.int32, (covars, covars), 0)
        lane = lax.broadcasted_iota(jnp.int32, (covars, covars), 1)
        right[...] = (row == lane).astype(jnp.float32)
        first_lane = lax.broadcasted_iota(jnp.int32, (1, covars), 1)
        first_row = lax.broadcasted_iota(jnp.int32, (covars, 1), 0)

        def body(i, _):
            g_row, r_row = gram[pl.ds(i, 1), :], right[pl.ds(i, 1), :]
            pivot = jnp.sum(jnp.where(first_lane == i, g_row, 0.0), axis=1, keepdims=True)
            g = gram[...]
            column = jnp.sum(jnp.where(lane == i, g, 0.0), axis=1, keepdims=True)
            factor = jnp.where(first_row > i, column / pivot, 0.0)
            lower[pl.ds(i, 1), :] = r_row
            lower_scaled[pl.ds(i, 1), :] = r_row / pivot
            gram[...] = g - factor * g_row
            right[...] = right[...] - factor * r_row
            return 0

        lax.fori_loop(0, covars, body, 0)

    def scan(chunk):
        rows = pl.ds(chunk * width, width)

        def load(j, total):
            return total + lax.dot_general(
                panel[rows, cut(j)], covs[:, cut(j)], columns,
                preferred_element_type=jnp.float32)

        loads = lax.fori_loop(0, spans, load, jnp.zeros((width, covars), jnp.float32))
        solved = lax.dot_general(loads, lower[...], columns, precision=lax.Precision.HIGHEST,
                                 preferred_element_type=jnp.float32)
        coeffs = jnp.dot(solved, lower_scaled[...], precision=lax.Precision.HIGHEST,
                         preferred_element_type=jnp.float32)
        parts = jnp.concatenate(terms(coeffs), axis=1)
        sq[...] = jnp.zeros_like(sq)

        def product(j, _):
            c = covs[:, cut(j)]
            fitted = jnp.dot(parts, jnp.concatenate([c, c, c], axis=0),
                             preferred_element_type=jnp.float32)
            resid = (panel[rows, cut(j)].astype(jnp.float32) - fitted).astype(jnp.bfloat16)
            wide = resid.astype(jnp.float32)
            sq[...] += jnp.sum(wide * wide, axis=1, keepdims=True)
            part = jnp.dot(resid, matched[cut(j), :], preferred_element_type=jnp.float32)

            @pl.when(j == 0)
            def _():
                out_ref[rows, :] = part

            @pl.when(j > 0)
            def _():
                out_ref[rows, :] += part
            return 0

        lax.fori_loop(0, spans, product, 0)
        out_ref[rows, :] = (scale * out_ref[rows, :] * lax.rsqrt(sq[...] + epsilon)
                            * lax.rsqrt(norm_ref[...] + epsilon))

    def stage(piece):
        for owner_z in range(depth):
            for owner_y in range(2):
                arrive(piece, index(owner_z, owner_y, 1 - core))
        if piece == 0:
            eliminate()
        else:
            scan(piece - 1)

    groups16 = samples // 16
    halves = [groups16 * p // 3 for p in range(4)]
    rest = expr_ref.shape[1] // lanes - 1
    widen(0)
    for piece in range(pieces):
        arrive(piece, y_peer)
        send(piece, y_peer, core_peer, dst(piece, y_peer))
        for src in z_from:
            arrive(piece, src)
            send(piece, src, y_peer, dst(piece, src))
            send(piece, src, core_peer, dst(piece, src))
        if piece:
            late(piece - 1)
        if piece < 3:
            match(0, halves[piece], halves[piece + 1])
        if piece == 2:
            for part in range(1, rest + 1):
                widen(part)
                match(part, 0, groups16)
        if piece >= 2:
            stage(piece - 2)
    stage(pieces - 2)
    late(pieces - 1)
    stage(pieces - 1)
    for copy in started:
        copy.wait_send()


def terms(x):
    first = x.astype(jnp.bfloat16)
    rest = x - first.astype(jnp.float32)
    second = rest.astype(jnp.bfloat16)
    return [first, second, (rest - second.astype(jnp.float32)).astype(jnp.bfloat16)]


def local(n, dosage, covariates, expression, block_index, expr_row):
    blocks, block_width = block_index.shape
    covars = covariates.shape[1]
    samples, genes = expression.shape
    variants = blocks * block_width
    scale = math.sqrt(samples - covars - 1)

    picked = jnp.take(dosage, block_index.reshape(-1), axis=1).T
    vmem = pl.BlockSpec(memory_space=pltpu.VMEM)
    depth = n // 4
    pieces = CHUNKS + 1
    sends = pieces * (depth - 1 + 2 + 1 + 2 * (depth - 1) + depth - 1)
    lanes = genes if samples * genes * 4 <= 2**23 else 128
    square = pltpu.VMEM((covars, covars), jnp.float32)
    return pl.pallas_call(
        functools.partial(exchange, n, scale),
        out_shape=jax.ShapeDtypeStruct((variants, genes), jnp.float32),
        in_specs=[vmem, vmem, vmem, pl.BlockSpec(memory_space=pltpu.SMEM)],
        out_specs=vmem,
        scratch_shapes=[
            pltpu.VMEM((variants, samples), jnp.bfloat16),
            pltpu.VMEM((covars, samples), jnp.bfloat16),
            pltpu.VMEM((samples, genes), jnp.bfloat16),
            pltpu.VMEM((samples, lanes), jnp.float32),
            pltpu.VMEM((16, lanes), jnp.float32),
            pltpu.VMEM((1, genes), jnp.float32),
            square, square, square, square,
            pltpu.VMEM((variants // CHUNKS, 1), jnp.float32),
            pltpu.SemaphoreType.DMA((sends,)),
            pltpu.SemaphoreType.DMA((pieces, n)),
        ],
        compiler_params=pltpu.CompilerParams(
            collective_id=0, has_side_effects=True, vmem_limit_bytes=63 * 2**20),
    )(picked, covariates.T, expression, expr_row)


def solution(mesh):
    placed = (
        P(("groups", "samp"), None),
        P(("groups", "samp"), None),
        P("groups", "samp"),
        P("groups", None),
        P("groups"),
    )
    return jax.shard_map(
        functools.partial(local, mesh.shape["samp"]),
        mesh=mesh, in_specs=placed, out_specs=P("groups", "samp"), check_vma=False
    )
```
